512 devices in a mesh: dp: 256 (over x, y, z), outer: 2 (over core).
Axes of the slice: x: 4, y: 8, z: 8, core: 2. Of those that a mesh axis runs over, the one named last changes fastest.
Arguments:
- gradient: float32 [512, 131072], P(('dp', 'outer')), may hold values from -6 to 6
- residual: float32 [512, 131072], P(('dp', 'outer')), may hold values from -6 to 6
- indices: int32 [512, 512], P(('dp', 'outer')), may hold values from 0 to 131071, as said below
- params: float32 [131072], replicated, may hold values from -6 to 6
Outputs:
- new_params: float32 [131072], replicated
- new_residual: float32 [512, 131072], P(('dp', 'outer'))
The draws below stay inside these ranges and needn't reach their ends.
Inputs may be any that keep to these rules, and one draw needn't show every extreme that they name: Within each worker's row the 512 indices are distinct and increasing: index j lies in [j * 256, (j + 1) * 256). Different workers often pick the same coordinate.
All inputs are finite; a program needn't handle non-finite values.
Results may differ from the reference program's by a relative error of at most 0.0003.
Values sent between devices are 32-bit elements.
No kernel may reach another device: no remote copies, remote signals or barrier semaphores. Data moves between devices by JAX's collectives and lax.ppermute only.
A program may use at most 64 MiB of HBM per device.

```python
import jax
import jax.numpy as jnp

PARAMS = 131072
DENSITY = 256
KEEP = 512
WORKERS = 512


def draw_indices(key, part):
    shared = jax.random.randint(jax.random.fold_in(key, 11), (1, KEEP), 0, DENSITY)
    others = jax.random.randint(jax.random.fold_in(key, 12), (WORKERS, KEEP), 0, DENSITY)
    picker = jax.random.randint(jax.random.fold_in(key, 13), (WORKERS, KEEP), 0, 4)
    offsets = jnp.where(picker == 0, shared, others)
    blocks = jnp.arange(KEEP, dtype=jnp.int32)[None, :] * DENSITY
    return (blocks + offsets).astype(jnp.int32)


def block_scale(rng, extent, shards, smallest, high):
    level, own = 1.0, jax.random.fold_in(rng, 6)
    for axis_at, parts in shards:
        draws = jnp.exp(jax.random.uniform(jax.random.fold_in(own, axis_at), (parts,), jnp.float32, smallest / len(shards), high / len(shards)))
        level = level * jnp.repeat(draws, extent[axis_at] // parts).reshape([-1 if axis == axis_at else 1 for axis in range(len(extent))])
    return level


def normal_values(key, extent, spread, most, pieces=(), held_as=jnp.bfloat16):
    gain = block_scale(key, extent, pieces, -0.22, 0.18) if pieces else 1.0
    result = jax.random.normal(key, extent, jnp.float32) * spread * gain
    return jnp.minimum(jnp.maximum(result, -most), most).astype(held_as)


def setup_inputs(seed: int = 0) -> dict:
    key_of = jax.random.split(jax.random.key(seed), 5)
    return {
        "gradient": normal_values(key_of[0], (WORKERS, PARAMS), 1.0, 6.0, ((0, 512),), jnp.float32),
        "residual": normal_values(key_of[1], (WORKERS, PARAMS), 0.5, 6.0, ((0, 512),), jnp.float32),
        "indices": draw_indices(jax.random.fold_in(key_of[4], 71), 0),
        "params": normal_values(key_of[3], (PARAMS,), 1.0, 6.0, (), jnp.float32),
    }


def reference(gradient, residual, indices, params):
    accumulated = gradient + residual
    sent = jnp.take_along_axis(accumulated, indices, axis=1)
    total = jnp.zeros((PARAMS,), jnp.float32).at[indices.reshape(-1)].add(sent.reshape(-1))
    new_params = params - 0.5 * total
    worker_rows = jnp.arange(WORKERS, dtype=jnp.int32)[:, None]
    new_residual = accumulated.at[worker_rows, indices].set(jnp.float32(0.0))
    return new_params, new_residual
```

```python
import jax
import jax.numpy as jnp
from jax import lax
from jax.experimental import pallas as pl
from jax.experimental.pallas import tpu as pltpu
from jax.sharding import Mesh
from jax.sharding import PartitionSpec as P

AXES = ("x1", "x0", "y2", "y1", "y0", "z2", "z1", "z0", "outer")
NEAR = ("x1", "x0")
FAR = tuple(a for a in AXES if a not in NEAR and a != "outer")
NS = 2 ** len(NEAR)
NT = 2 ** len(FAR)
NB = 256 // NS
PACK = 64 // NB
STEP = 0.5


def lanes(shape):
    return lax.broadcasted_iota(jnp.int32, shape, 1)


def pick_kernel(idx_ref, g_ref, r_ref, send_ref, res_ref, v_scr, o_scr):
    step = pl.program_id(0)
    off = (idx_ref[pl.ds(step, 1), :] & 255).astype(jnp.float32)
    col = jnp.transpose(jnp.broadcast_to(off, (128, 128)))
    lane = lanes((128, 128)).astype(jnp.float32)
    low = col == lane
    high = col == lane + 128.0
    even = pl.ds(0, 128, stride=2)
    odd = pl.ds(1, 128, stride=2)
    a0 = g_ref[even, :] + r_ref[even, :]
    a1 = g_ref[odd, :] + r_ref[odd, :]
    res_ref[even, :] = jnp.where(low, 0.0, a0)
    res_ref[odd, :] = jnp.where(high, 0.0, a1)
    hit = jnp.where(low, a0, jnp.where(high, a1, 0.0))
    v_scr[pl.ds(step, 1), :] = jnp.sum(jnp.transpose(hit), axis=0, keepdims=True)
    o_scr[pl.ds(step, 1), :] = off

    @pl.when(step == 3)
    def _():
        lane1 = lanes((1, 128))
        for s in range(NS):
            for c in range(2):
                block = c * 256 + s * NB
                row, at = block // 128, block % 128
                val = v_scr[row : row + 1, :]
                offs = o_scr[row : row + 1, :]
                left = pltpu.roll(val, (128 - at) % 128, 1) if at else val
                move = (NB - at) % 128
                right = pltpu.roll(offs, move, 1) if move else offs
                send_ref[s * 2 + c] = jnp.where(lane1 < NB, left, right)[:, : 2 * NB]


def pick(idx, g, r):
    return pl.pallas_call(
        pick_kernel,
        grid=(4,),
        in_specs=[
            pl.BlockSpec((4, 128), lambda i: (0, 0)),
            pl.BlockSpec((256, 128), lambda i: (i, 0)),
            pl.BlockSpec((256, 128), lambda i: (i, 0)),
        ],
        out_specs=[
            pl.BlockSpec((2 * NS, 1, 2 * NB), lambda i: (0, 0, 0)),
            pl.BlockSpec((256, 128), lambda i: (i, 0)),
        ],
        out_shape=[
            jax.ShapeDtypeStruct((2 * NS, 1, 2 * NB), jnp.float32),
            jax.ShapeDtypeStruct((1024, 128), jnp.float32),
        ],
        scratch_shapes=[pltpu.VMEM((4, 128), jnp.float32), pltpu.VMEM((4, 128), jnp.float32)],
        name="pick",
    )(idx, g, r)


def copies_kernel(in_ref, out_ref, scr):
    for p in range(8):
        rows = [in_ref[p + 8 * i] for i in range(PACK)]
        scr[p : p + 1, :] = rows[0] if PACK == 1 else jnp.concatenate(rows, axis=1)
    whole = scr[...]
    for t in range(NT):
        out_ref[t] = whole


def copies(pairs):
    return pl.pallas_call(
        copies_kernel,
        out_shape=jax.ShapeDtypeStruct((NT, 8, 128), jnp.float32),
        scratch_shapes=[pltpu.VMEM((8, 128), jnp.float32)],
        name="copies",
    )(pairs)


GROUP = 8


def total_kernel(where_ref, w_ref, p_ref, out_ref, tot):
    lane = lanes((8, 128)).astype(jnp.float32)
    lane_high = lane + 128.0
    for k0 in range(0, NB, GROUP):

        def body(t, accs):
            w = w_ref[t]
            accs = list(accs)
            for i in range(PACK):
                for k in range(GROUP):
                    at = i * 2 * NB + k0 + k
                    val = jnp.broadcast_to(w[:, at : at + 1], (8, 128))
                    off = jnp.broadcast_to(w[:, at + NB : at + NB + 1], (8, 128))
                    accs[2 * k] += jnp.where(off == lane, val, 0.0)
                    accs[2 * k + 1] += jnp.where(off == lane_high, val, 0.0)
            return tuple(accs)

        accs = lax.fori_loop(0, NT, body, (jnp.zeros((8, 128), jnp.float32),) * (2 * GROUP))
        for n, acc in enumerate(accs):
            tot[2 * k0 + n : 2 * k0 + n + 1, :] = jnp.sum(acc, axis=0, keepdims=True)
    new = p_ref[...] - STEP * tot[...]
    for s in range(NS):
        out_ref[s] = new


def total(where, pairs, params):
    rows = 2 * NB
    return pl.pallas_call(
        total_kernel,
        grid_spec=pltpu.PrefetchScalarGridSpec(
            num_scalar_prefetch=1,
            grid=(1,),
            in_specs=[
                pl.BlockSpec((NT, 8, 128), lambda i, at: (0, 0, 0)),
                pl.BlockSpec((rows, 128), lambda i, at: (at[0], 0)),
            ],
            out_specs=pl.BlockSpec((NS, rows, 128), lambda i, at: (0, 0, 0)),
            scratch_shapes=[pltpu.VMEM((rows, 128), jnp.float32)],
        ),
        out_shape=jax.ShapeDtypeStruct((NS, rows, 128), jnp.float32),
        name="total",
    )(where, pairs, params)


def shards(gradient, residual, indices, params):
    g = gradient.reshape(1024, 128)
    r = residual.reshape(1024, 128)
    idx = indices.reshape(4, 128)
    send, res = pick(idx, g, r)
    got = lax.all_to_all(send, NEAR + ("outer",), 0, 0)
    everyone = lax.all_to_all(copies(got), FAR, 0, 0)
    where = lax.axis_index("outer") * NS + lax.axis_index(NEAR)
    new = total(where.reshape(1).astype(jnp.int32), everyone, params.reshape(1024, 128))
    half = lax.all_to_all(new, NEAR, 0, 0)
    both = lax.all_gather(half.reshape(512, 128), "outer", axis=0, tiled=True)
    return both.reshape(131072), res.reshape(1, 131072)


def solution(mesh):
    torus = Mesh(mesh.devices.reshape((2,) * 9), AXES)
    placed = (P(AXES, None), P(AXES, None), P(AXES, None), P())
    return jax.shard_map(
        shards, mesh=torus, in_specs=placed, out_specs=(P(), P(AXES, None)), check_vma=False
    )
```

```python
import jax
import jax.numpy as jnp
from jax import lax
from jax.experimental import pallas as pl
from jax.experimental.pallas import tpu as pltpu
from jax.sharding import Mesh
from jax.sharding import PartitionSpec as P

AXES = ("x1", "x0", "y2", "y1", "y0", "z2", "z1", "z0", "outer")
NEAR = ("x1", "x0")
FAR = tuple(a for a in AXES if a not in NEAR and a != "outer")
NS = 2 ** len(NEAR)
NT = 2 ** len(FAR)
NB = 256 // NS
PACK = 64 // NB
STEP = 0.5


def lanes(shape):
    return lax.broadcasted_iota(jnp.int32, shape, 1)


def pick_kernel(idx_ref, g_ref, r_ref, send_ref, res_ref, v_scr, o_scr):
    step = pl.program_id(0)
    off = (idx_ref[pl.ds(step, 1), :] & 255).astype(jnp.float32)
    col = jnp.transpose(jnp.broadcast_to(off, (128, 128)))
    lane = lanes((128, 128)).astype(jnp.float32)
    low = col == lane
    high = col == lane + 128.0
    even = pl.ds(0, 128, stride=2)
    odd = pl.ds(1, 128, stride=2)
    a0 = g_ref[even, :] + r_ref[even, :]
    a1 = g_ref[odd, :] + r_ref[odd, :]
    res_ref[even, :] = jnp.where(low, 0.0, a0)
    res_ref[odd, :] = jnp.where(high, 0.0, a1)
    hit = jnp.where(low, a0, jnp.where(high, a1, 0.0))
    v_scr[pl.ds(step, 1), :] = jnp.sum(jnp.transpose(hit), axis=0, keepdims=True)
    o_scr[pl.ds(step, 1), :] = off

    @pl.when(step == 3)
    def _():
        lane1 = lanes((1, 128))
        for s in range(NS):
            for c in range(2):
                block = c * 256 + s * NB
                row, at = block // 128, block % 128
                val = v_scr[row : row + 1, :]
                offs = o_scr[row : row + 1, :]
                left = pltpu.roll(val, (128 - at) % 128, 1) if at else val
                move = (NB - at) % 128
                right = pltpu.roll(offs, move, 1) if move else offs
                send_ref[s * 2 + c] = jnp.where(lane1 < NB, left, right)[:, : 2 * NB]


def pick(idx, g, r):
    return pl.pallas_call(
        pick_kernel,
        grid=(4,),
        in_specs=[
            pl.BlockSpec((4, 128), lambda i: (0, 0)),
            pl.BlockSpec((256, 128), lambda i: (i, 0)),
            pl.BlockSpec((256, 128), lambda i: (i, 0)),
        ],
        out_specs=[
            pl.BlockSpec((2 * NS, 1, 2 * NB), lambda i: (0, 0, 0)),
            pl.BlockSpec((256, 128), lambda i: (i, 0)),
        ],
        out_shape=[
            pltpu.VMEM((2 * NS, 1, 2 * NB), jnp.float32),
            jax.ShapeDtypeStruct((1024, 128), jnp.float32),
        ],
        scratch_shapes=[pltpu.VMEM((4, 128), jnp.float32), pltpu.VMEM((4, 128), jnp.float32)],
        name="pick",
    )(idx, g, r)


def copies_kernel(in_ref, out_ref, scr):
    for p in range(8):
        rows = [in_ref[p + 8 * i] for i in range(PACK)]
        scr[p : p + 1, :] = rows[0] if PACK == 1 else jnp.concatenate(rows, axis=1)
    whole = scr[...]
    for t in range(NT):
        out_ref[t] = whole


def near(x):
    return pltpu.with_memory_space_constraint(x, pltpu.VMEM)


def copies(pairs):
    return pl.pallas_call(
        copies_kernel,
        out_shape=pltpu.VMEM((NT, 8, 128), jnp.float32),
        scratch_shapes=[pltpu.VMEM((8, 128), jnp.float32)],
        name="copies",
    )(near(pairs))


GROUP = 8
ROWS = 512 // PACK


def total_kernel(where_ref, w_ref, p_ref, out_ref, turned, tot):
    whole = w_ref[...].reshape(ROWS, 128)
    for n in range(ROWS // 128):
        turned[:, 128 * n : 128 * n + 128] = jnp.transpose(whole[128 * n : 128 * n + 128, :])
    digit = lax.broadcasted_iota(jnp.int32, (16, ROWS), 0).astype(jnp.float32)
    row = lax.broadcasted_iota(jnp.int32, (128, 128), 0)
    lane = lanes((128, 128))
    own = (row // 16) == (lane // 16)
    spot = (row % 8) == (lane // 16)
    for k0 in range(0, NB, GROUP):
        acc = jnp.zeros((128, 128), jnp.float32)
        for i in range(PACK):
            parts = ([], [], [])
            right = []
            at = i * 2 * NB + k0
            val = turned[at : at + GROUP, :]
            off = turned[at + NB : at + NB + GROUP, :]
            first = val.astype(jnp.bfloat16).astype(jnp.float32)
            rest = val - first
            second = rest.astype(jnp.bfloat16).astype(jnp.float32)
            third = rest - second
            hi = jnp.floor(off * 0.0625)
            lo = off - 16.0 * hi
            for k in range(GROUP):
                hot = digit == hi[k : k + 1, :]
                for m, part in enumerate((first, second, third)):
                    parts[m].append(jnp.where(hot, part[k : k + 1, :], 0.0).astype(jnp.bfloat16))
                right.append(jnp.where(digit == lo[k : k + 1, :], 1.0, 0.0).astype(jnp.bfloat16))
            right = jnp.concatenate(right, axis=0)
            for m in range(3):
                acc += lax.dot_general(
                    jnp.concatenate(parts[m], axis=0),
                    right,
                    (((1,), (1,)), ((), ())),
                    preferred_element_type=jnp.float32,
                )
        acc = jnp.where(own, acc, 0.0)
        for turn in (64, 32, 16):
            acc = acc + pltpu.roll(acc, turn, 1)
        acc = jnp.where(spot, acc, 0.0)
        tot[2 * k0 : 2 * k0 + 16, :] = jnp.sum(acc.reshape(16, 8, 128), axis=1)
    new = p_ref[...] - STEP * tot[...]
    for s in range(NS):
        out_ref[s] = new


def total(where, pairs, params):
    rows = 2 * NB
    return pl.pallas_call(
        total_kernel,
        grid_spec=pltpu.PrefetchScalarGridSpec(
            num_scalar_prefetch=1,
            grid=(1,),
            in_specs=[
                pl.BlockSpec((NT, 8, 128), lambda i, at: (0, 0, 0)),
                pl.BlockSpec((rows, 128), lambda i, at: (at[0], 0)),
            ],
            out_specs=pl.BlockSpec((NS, rows, 128), lambda i, at: (0, 0, 0)),
            scratch_shapes=[pltpu.VMEM((128, ROWS), jnp.float32), pltpu.VMEM((rows, 128), jnp.float32)],
        ),
        out_shape=pltpu.VMEM((NS, rows, 128), jnp.float32),
        name="total",
    )(where, near(pairs), params)


def shards(gradient, residual, indices, params):
    g = gradient.reshape(1024, 128)
    r = residual.reshape(1024, 128)
    idx = indices.reshape(4, 128)
    where = (lax.axis_index("outer") * NS + lax.axis_index(NEAR)).reshape(1).astype(jnp.int32)
    where, idx = lax.optimization_barrier((where, idx))
    send, res = pick(idx, g, r)
    got = lax.all_to_all(send, NEAR + ("outer",), 0, 0)
    everyone = lax.all_to_all(copies(got), FAR, 0, 0)
    new = total(where, everyone, params.reshape(1024, 128))
    half = lax.all_to_all(new, NEAR, 0, 0)
    both = lax.all_gather(half.reshape(512, 128), "outer", axis=0, tiled=True)
    return both.reshape(131072), res.reshape(1, 131072)


def solution(mesh):
    torus = Mesh(mesh.devices.reshape((2,) * 9), AXES)
    placed = (P(AXES, None), P(AXES, None), P(AXES, None), P())
    return jax.shard_map(
        shards, mesh=torus, in_specs=placed, out_specs=(P(), P(AXES, None)), check_vma=False
    )
```

```python
import jax
import jax.numpy as jnp
from jax import lax
from jax.experimental import pallas as pl
from jax.experimental.pallas import tpu as pltpu
from jax.sharding import Mesh
from jax.sharding import PartitionSpec as P

AXES = ("x1", "x0", "y2", "y1", "y0", "z2", "z1", "z0", "outer")
NEAR = ("x1", "x0")
FAR = tuple(a for a in AXES if a not in NEAR and a != "outer")
NS = 2 ** len(NEAR)
NT = 2 ** len(FAR)
NB = 256 // NS
PACK = 64 // NB
STEP = 0.5


def lanes(shape):
    return lax.broadcasted_iota(jnp.int32, shape, 1)


def pick_kernel(idx_ref, g_hbm, r_hbm, send_ref, res_hbm, g_ref, r_ref, res_ref, v_scr, o_scr, col_scr, g_sem, r_sem, res_sem):
    def span(n):
        return pl.ds(256 * n, 256)

    loads = []
    for n in range(4):
        one = pltpu.make_async_copy(g_hbm.at[span(n)], g_ref.at[span(n)], g_sem.at[n])
        two = pltpu.make_async_copy(r_hbm.at[span(n)], r_ref.at[span(n)], r_sem.at[n])
        one.start()
        two.start()
        loads.append((one, two))
    for n in range(4):
        off = (idx_ref[n : n + 1, :] & 255).astype(jnp.float32)
        o_scr[n : n + 1, :] = off
        col_scr[n] = jnp.transpose(jnp.broadcast_to(off, (128, 128)))
    lane = lanes((128, 128)).astype(jnp.float32)
    stores = []
    for n in range(4):
        for load in loads[n]:
            load.wait()
        col = col_scr[n]
        low = col == lane
        high = col == lane + 128.0
        even = pl.ds(256 * n, 128, stride=2)
        odd = pl.ds(256 * n + 1, 128, stride=2)
        a0 = g_ref[even, :] + r_ref[even, :]
        a1 = g_ref[odd, :] + r_ref[odd, :]
        res_ref[even, :] = jnp.where(low, 0.0, a0)
        res_ref[odd, :] = jnp.where(high, 0.0, a1)
        store = pltpu.make_async_copy(res_ref.at[span(n)], res_hbm.at[span(n)], res_sem.at[n])
        store.start()
        stores.append(store)
        hit = jnp.where(low, a0, jnp.where(high, a1, 0.0))
        v_scr[n : n + 1, :] = jnp.sum(jnp.transpose(hit), axis=0, keepdims=True)
    lane1 = lanes((1, 128))
    for s in range(NS):
        for c in range(2):
            block = c * 256 + s * NB
            row, at = block // 128, block % 128
            val = v_scr[row : row + 1, :]
            offs = o_scr[row : row + 1, :]
            left = pltpu.roll(val, (128 - at) % 128, 1) if at else val
            move = (NB - at) % 128
            right = pltpu.roll(offs, move, 1) if move else offs
            send_ref[s * 2 + c] = jnp.where(lane1 < NB, left, right)[:, : 2 * NB]
    for store in stores:
        store.wait()


def pick(idx, g, r):
    in_hbm = pl.BlockSpec(memory_space=pltpu.HBM)
    in_vmem = pl.BlockSpec(memory_space=pltpu.VMEM)
    return pl.pallas_call(
        pick_kernel,
        in_specs=[in_vmem, in_hbm, in_hbm],
        out_specs=[in_vmem, in_hbm],
        out_shape=[
            pltpu.VMEM((2 * NS, 1, 2 * NB), jnp.float32),
            jax.ShapeDtypeStruct((1024, 128), jnp.float32),
        ],
        scratch_shapes=[
            pltpu.VMEM((1024, 128), jnp.float32),
            pltpu.VMEM((1024, 128), jnp.float32),
            pltpu.VMEM((1024, 128), jnp.float32),
            pltpu.VMEM((4, 128), jnp.float32),
            pltpu.VMEM((4, 128), jnp.float32),
            pltpu.VMEM((4, 128, 128), jnp.float32),
            pltpu.SemaphoreType.DMA((4,)),
            pltpu.SemaphoreType.DMA((4,)),
            pltpu.SemaphoreType.DMA((4,)),
        ],
        name="pick",
    )(idx, g, r)


def copies_kernel(in_ref, out_ref, scr):
    for p in range(8):
        rows = [in_ref[p + 8 * i] for i in range(PACK)]
        scr[p : p + 1, :] = rows[0] if PACK == 1 else jnp.concatenate(rows, axis=1)
    whole = scr[...]
    for t in range(NT):
        out_ref[t] = whole


def near(x):
    return pltpu.with_memory_space_constraint(x, pltpu.VMEM)


def copies(pairs):
    return pl.pallas_call(
        copies_kernel,
        out_shape=pltpu.VMEM((NT, 8, 128), jnp.float32),
        scratch_shapes=[pltpu.VMEM((8, 128), jnp.float32)],
        name="copies",
    )(near(pairs))


GROUP = 8
ROWS = 512 // PACK


def total_kernel(where_ref, w_ref, p_ref, out_ref, turned, tot):
    whole = w_ref[...].reshape(ROWS, 128)
    for n in range(ROWS // 128):
        turned[:, 128 * n : 128 * n + 128] = jnp.transpose(whole[128 * n : 128 * n + 128, :])
    digit = lax.broadcasted_iota(jnp.int32, (16, ROWS), 0).astype(jnp.float32)
    row = lax.broadcasted_iota(jnp.int32, (128, 128), 0)
    lane = lanes((128, 128))
    own = (row // 16) == (lane // 16)
    spot = (row % 8) == (lane // 16)
    for k0 in range(0, NB, GROUP):
        acc = jnp.zeros((128, 128), jnp.float32)
        for i in range(PACK):
            parts = ([], [], [])
            right = []
            at = i * 2 * NB + k0
            val = turned[at : at + GROUP, :]
            off = turned[at + NB : at + NB + GROUP, :]
            first = val.astype(jnp.bfloat16).astype(jnp.float32)
            rest = val - first
            second = rest.astype(jnp.bfloat16).astype(jnp.float32)
            third = rest - second
            hi = jnp.floor(off * 0.0625)
            lo = off - 16.0 * hi
            for k in range(GROUP):
                hot = digit == hi[k : k + 1, :]
                for m, part in enumerate((first, second, third)):
                    parts[m].append(jnp.where(hot, part[k : k + 1, :], 0.0).astype(jnp.bfloat16))
                right.append(jnp.where(digit == lo[k : k + 1, :], 1.0, 0.0).astype(jnp.bfloat16))
            right = jnp.concatenate(right, axis=0)
            for m in range(3):
                acc += lax.dot_general(
                    jnp.concatenate(parts[m], axis=0),
                    right,
                    (((1,), (1,)), ((), ())),
                    preferred_element_type=jnp.float32,
                )
        acc = jnp.where(own, acc, 0.0)
        for turn in (64, 32, 16):
            acc = acc + pltpu.roll(acc, turn, 1)
        acc = jnp.where(spot, acc, 0.0)
        tot[2 * k0 : 2 * k0 + 16, :] = jnp.sum(acc.reshape(16, 8, 128), axis=1)
    new = p_ref[...] - STEP * tot[...]
    for s in range(NS):
        out_ref[s] = new


def total(where, pairs, params):
    rows = 2 * NB
    return pl.pallas_call(
        total_kernel,
        grid_spec=pltpu.PrefetchScalarGridSpec(
            num_scalar_prefetch=1,
            grid=(1,),
            in_specs=[
                pl.BlockSpec((NT, 8, 128), lambda i, at: (0, 0, 0)),
                pl.BlockSpec((rows, 128), lambda i, at: (at[0], 0)),
            ],
            out_specs=pl.BlockSpec((NS, rows, 128), lambda i, at: (0, 0, 0)),
            scratch_shapes=[pltpu.VMEM((128, ROWS), jnp.float32), pltpu.VMEM((rows, 128), jnp.float32)],
        ),
        out_shape=pltpu.VMEM((NS, rows, 128), jnp.float32),
        name="total",
    )(where, near(pairs), params)


def shards(gradient, residual, indices, params):
    g = gradient.reshape(1024, 128)
    r = residual.reshape(1024, 128)
    idx = indices.reshape(4, 128)
    where = (lax.axis_index("outer") * NS + lax.axis_index(NEAR)).reshape(1).astype(jnp.int32)
    where, idx = lax.optimization_barrier((where, idx))
    send, res = pick(idx, g, r)
    got = lax.all_to_all(send, NEAR + ("outer",), 0, 0)
    everyone = lax.all_to_all(copies(got), FAR, 0, 0)
    new = total(where, everyone, params.reshape(1024, 128))
    half = lax.all_to_all(new, NEAR, 0, 0)
    both = lax.all_gather(half.reshape(512, 128), "outer", axis=0, tiled=True)
    return both.reshape(131072), res.reshape(1, 131072)


def solution(mesh):
    torus = Mesh(mesh.devices.reshape((2,) * 9), AXES)
    placed = (P(AXES, None), P(AXES, None), P(AXES, None), P())
    return jax.shard_map(
        shards, mesh=torus, in_specs=placed, out_specs=(P(), P(AXES, None)), check_vma=False
    )
```

```python
import jax
import jax.numpy as jnp
from jax import lax
from jax.experimental import pallas as pl
from jax.experimental.pallas import tpu as pltpu
from jax.sharding import Mesh
from jax.sharding import PartitionSpec as P

AXES = ("x1", "x0", "y2", "y1", "y0", "z2", "z1", "z0", "outer")
NEAR = ("x1", "x0", "y0")
FAR = tuple(a for a in AXES if a not in NEAR and a != "outer")
NS = 2 ** len(NEAR)
NT = 2 ** len(FAR)
NB = 256 // NS
PACK = 64 // NB
STEP = 0.5


def lanes(shape):
    return lax.broadcasted_iota(jnp.int32, shape, 1)


def pick_kernel(idx_ref, g_hbm, r_hbm, send_ref, res_hbm, g_ref, r_ref, res_ref, v_scr, o_scr, col_scr, g_sem, r_sem, res_sem):
    def span(n):
        return pl.ds(256 * n, 256)

    loads = []
    for n in range(4):
        one = pltpu.make_async_copy(g_hbm.at[span(n)], g_ref.at[span(n)], g_sem.at[n])
        two = pltpu.make_async_copy(r_hbm.at[span(n)], r_ref.at[span(n)], r_sem.at[n])
        one.start()
        two.start()
        loads.append((one, two))
    for n in range(4):
        off = (idx_ref[n : n + 1, :] & 255).astype(jnp.float32)
        o_scr[n : n + 1, :] = off
        col_scr[n] = jnp.transpose(jnp.broadcast_to(off, (128, 128)))
    lane = lanes((128, 128)).astype(jnp.float32)
    stores = []
    for n in range(4):
        for load in loads[n]:
            load.wait()
        col = col_scr[n]
        low = col == lane
        high = col == lane + 128.0
        even = pl.ds(256 * n, 128, stride=2)
        odd = pl.ds(256 * n + 1, 128, stride=2)
        a0 = g_ref[even, :] + r_ref[even, :]
        a1 = g_ref[odd, :] + r_ref[odd, :]
        res_ref[even, :] = jnp.where(low, 0.0, a0)
        res_ref[odd, :] = jnp.where(high, 0.0, a1)
        store = pltpu.make_async_copy(res_ref.at[span(n)], res_hbm.at[span(n)], res_sem.at[n])
        store.start()
        stores.append(store)
        hit = jnp.where(low, a0, jnp.where(high, a1, 0.0))
        v_scr[n : n + 1, :] = jnp.sum(jnp.transpose(hit), axis=0, keepdims=True)
    lane1 = lanes((1, 128))
    for s in range(NS):
        for c in range(2):
            block = c * 256 + s * NB
            row, at = block // 128, block % 128
            val = v_scr[row : row + 1, :]
            offs = o_scr[row : row + 1, :]
            left = pltpu.roll(val, (128 - at) % 128, 1) if at else val
            move = (NB - at) % 128
            right = pltpu.roll(offs, move, 1) if move else offs
            send_ref[s * 2 + c] = jnp.where(lane1 < NB, left, right)[:, : 2 * NB]
    for store in stores:
        store.wait()


def pick(idx, g, r):
    in_hbm = pl.BlockSpec(memory_space=pltpu.HBM)
    in_vmem = pl.BlockSpec(memory_space=pltpu.VMEM)
    return pl.pallas_call(
        pick_kernel,
        in_specs=[in_vmem, in_hbm, in_hbm],
        out_specs=[in_vmem, in_hbm],
        out_shape=[
            pltpu.VMEM((2 * NS, 1, 2 * NB), jnp.float32),
            jax.ShapeDtypeStruct((1024, 128), jnp.float32),
        ],
        scratch_shapes=[
            pltpu.VMEM((1024, 128), jnp.float32),
            pltpu.VMEM((1024, 128), jnp.float32),
            pltpu.VMEM((1024, 128), jnp.float32),
            pltpu.VMEM((4, 128), jnp.float32),
            pltpu.VMEM((4, 128), jnp.float32),
            pltpu.VMEM((4, 128, 128), jnp.float32),
            pltpu.SemaphoreType.DMA((4,)),
            pltpu.SemaphoreType.DMA((4,)),
            pltpu.SemaphoreType.DMA((4,)),
        ],
        name="pick",
    )(idx, g, r)


def copies_kernel(in_ref, out_ref, scr):
    for p in range(8):
        rows = [in_ref[p + 8 * i] for i in range(PACK)]
        scr[p : p + 1, :] = rows[0] if PACK == 1 else jnp.concatenate(rows, axis=1)
    whole = scr[...]
    for t in range(NT):
        out_ref[t] = whole


def near(x):
    return pltpu.with_memory_space_constraint(x, pltpu.VMEM)


def copies(pairs):
    return pl.pallas_call(
        copies_kernel,
        out_shape=pltpu.VMEM((NT, 8, 128), jnp.float32),
        scratch_shapes=[pltpu.VMEM((8, 128), jnp.float32)],
        name="copies",
    )(near(pairs))


GROUP = 8
ROWS = 512 // PACK


def total_kernel(where_ref, w_ref, p_ref, out_ref, turned, tot):
    whole = w_ref[...].reshape(ROWS, 128)
    for n in range(ROWS // 128):
        turned[:, 128 * n : 128 * n + 128] = jnp.transpose(whole[128 * n : 128 * n + 128, :])
    digit = lax.broadcasted_iota(jnp.int32, (16, ROWS), 0).astype(jnp.float32)
    row = lax.broadcasted_iota(jnp.int32, (128, 128), 0)
    lane = lanes((128, 128))
    own = (row // 16) == (lane // 16)
    spot = (row % 8) == (lane // 16)
    for k0 in range(0, NB, GROUP):
        acc = jnp.zeros((128, 128), jnp.float32)
        for i in range(PACK):
            parts = ([], [], [])
            right = []
            at = i * 2 * NB + k0
            val = turned[at : at + GROUP, :]
            off = turned[at + NB : at + NB + GROUP, :]
            first = val.astype(jnp.bfloat16).astype(jnp.float32)
            rest = val - first
            second = rest.astype(jnp.bfloat16).astype(jnp.float32)
            third = rest - second
            hi = jnp.floor(off * 0.0625)
            lo = off - 16.0 * hi
            for k in range(GROUP):
                hot = digit == hi[k : k + 1, :]
                for m, part in enumerate((first, second, third)):
                    parts[m].append(jnp.where(hot, part[k : k + 1, :], 0.0).astype(jnp.bfloat16))
                right.append(jnp.where(digit == lo[k : k + 1, :], 1.0, 0.0).astype(jnp.bfloat16))
            right = jnp.concatenate(right, axis=0)
            for m in range(3):
                acc += lax.dot_general(
                    jnp.concatenate(parts[m], axis=0),
                    right,
                    (((1,), (1,)), ((), ())),
                    preferred_element_type=jnp.float32,
                )
        acc = jnp.where(own, acc, 0.0)
        for turn in (64, 32, 16):
            acc = acc + pltpu.roll(acc, turn, 1)
        acc = jnp.where(spot, acc, 0.0)
        tot[2 * k0 : 2 * k0 + 16, :] = jnp.sum(acc.reshape(16, 8, 128), axis=1)
    new = p_ref[...] - STEP * tot[...]
    for s in range(NS):
        out_ref[s] = new


def total(where, pairs, params):
    rows = 2 * NB
    return pl.pallas_call(
        total_kernel,
        grid_spec=pltpu.PrefetchScalarGridSpec(
            num_scalar_prefetch=1,
            grid=(1,),
            in_specs=[
                pl.BlockSpec((NT, 8, 128), lambda i, at: (0, 0, 0)),
                pl.BlockSpec((rows, 128), lambda i, at: (at[0], 0)),
            ],
            out_specs=pl.BlockSpec((NS, rows, 128), lambda i, at: (0, 0, 0)),
            scratch_shapes=[pltpu.VMEM((128, ROWS), jnp.float32), pltpu.VMEM((rows, 128), jnp.float32)],
        ),
        out_shape=pltpu.VMEM((NS, rows, 128), jnp.float32),
        name="total",
    )(where, near(pairs), params)


def shards(gradient, residual, indices, params):
    g = gradient.reshape(1024, 128)
    r = residual.reshape(1024, 128)
    idx = indices.reshape(4, 128)
    where = (lax.axis_index("outer") * NS + lax.axis_index(NEAR)).reshape(1).astype(jnp.int32)
    where, idx = lax.optimization_barrier((where, idx))
    send, res = pick(idx, g, r)
    got = lax.all_to_all(send, NEAR + ("outer",), 0, 0)
    everyone = lax.all_to_all(copies(got), FAR, 0, 0)
    new = total(where, everyone, params.reshape(1024, 128))
    half = lax.all_to_all(new, NEAR, 0, 0)
    both = lax.all_gather(half.reshape(512, 128), "outer", axis=0, tiled=True)
    return both.reshape(131072), res.reshape(1, 131072)


def solution(mesh):
    torus = Mesh(mesh.devices.reshape((2,) * 9), AXES)
    placed = (P(AXES, None), P(AXES, None), P(AXES, None), P())
    return jax.shard_map(
        shards, mesh=torus, in_specs=placed, out_specs=(P(), P(AXES, None)), check_vma=False
    )
```

```python
import jax
import jax.numpy as jnp
from jax import lax
from jax.experimental import pallas as pl
from jax.experimental.pallas import tpu as pltpu
from jax.sharding import Mesh
from jax.sharding import PartitionSpec as P

AXES = ("x1", "x0", "y2", "y1", "y0", "z2", "z1", "z0", "outer")
NEAR = ("x1", "x0", "y0")
FAR = tuple(a for a in AXES if a not in NEAR and a != "outer")
NS = 2 ** len(NEAR)
NT = 2 ** len(FAR)
NB = 256 // NS
PACK = 64 // NB
STEP = 0.5


def lanes(shape):
    return lax.broadcasted_iota(jnp.int32, shape, 1)


def pick_kernel(idx_ref, g_hbm, r_hbm, send_ref, res_hbm, g_ref, r_ref, res_ref, v_scr, o_scr, col_scr, g_sem, r_sem, res_sem):
    def span(n):
        return pl.ds(256 * n, 256)

    loads = []
    for n in range(4):
        one = pltpu.make_async_copy(g_hbm.at[span(n)], g_ref.at[span(n)], g_sem.at[n])
        two = pltpu.make_async_copy(r_hbm.at[span(n)], r_ref.at[span(n)], r_sem.at[n])
        one.start()
        two.start()
        loads.append((one, two))
    for n in range(4):
        off = (idx_ref[n : n + 1, :] & 255).astype(jnp.float32)
        o_scr[n : n + 1, :] = off
        col_scr[n] = jnp.transpose(jnp.broadcast_to(off, (128, 128)))
    lane = lanes((128, 128)).astype(jnp.float32)
    stores = []
    for n in range(4):
        for load in loads[n]:
            load.wait()
        col = col_scr[n]
        low = col == lane
        high = col == lane + 128.0
        even = pl.ds(256 * n, 128, stride=2)
        odd = pl.ds(256 * n + 1, 128, stride=2)
        a0 = g_ref[even, :] + r_ref[even, :]
        a1 = g_ref[odd, :] + r_ref[odd, :]
        res_ref[even, :] = jnp.where(low, 0.0, a0)
        res_ref[odd, :] = jnp.where(high, 0.0, a1)
        store = pltpu.make_async_copy(res_ref.at[span(n)], res_hbm.at[span(n)], res_sem.at[n])
        store.start()
        stores.append(store)
        hit = jnp.where(low, a0, jnp.where(high, a1, 0.0))
        v_scr[n : n + 1, :] = jnp.sum(jnp.transpose(hit), axis=0, keepdims=True)
    lane1 = lanes((1, 128))
    for s in range(NS):
        for c in range(2):
            block = c * 256 + s * NB
            row, at = block // 128, block % 128
            val = v_scr[row : row + 1, :]
            offs = o_scr[row : row + 1, :]
            left = pltpu.roll(val, (128 - at) % 128, 1) if at else val
            move = (NB - at) % 128
            right = pltpu.roll(offs, move, 1) if move else offs
            send_ref[s * 2 + c] = jnp.where(lane1 < NB, left, right)[:, : 2 * NB]
    for store in stores:
        store.wait()


def pick(idx, g, r):
    in_hbm = pl.BlockSpec(memory_space=pltpu.HBM)
    in_vmem = pl.BlockSpec(memory_space=pltpu.VMEM)
    return pl.pallas_call(
        pick_kernel,
        in_specs=[in_vmem, in_hbm, in_hbm],
        out_specs=[in_vmem, in_hbm],
        out_shape=[
            pltpu.VMEM((2 * NS, 1, 2 * NB), jnp.float32),
            jax.ShapeDtypeStruct((1024, 128), jnp.float32),
        ],
        scratch_shapes=[
            pltpu.VMEM((1024, 128), jnp.float32),
            pltpu.VMEM((1024, 128), jnp.float32),
            pltpu.VMEM((1024, 128), jnp.float32),
            pltpu.VMEM((4, 128), jnp.float32),
            pltpu.VMEM((4, 128), jnp.float32),
            pltpu.VMEM((4, 128, 128), jnp.float32),
            pltpu.SemaphoreType.DMA((4,)),
            pltpu.SemaphoreType.DMA((4,)),
            pltpu.SemaphoreType.DMA((4,)),
        ],
        name="pick",
    )(idx, g, r)


def copies_kernel(in_ref, out_ref, scr):
    for p in range(8):
        rows = [in_ref[p + 8 * i] for i in range(PACK)]
        scr[p : p + 1, :] = rows[0] if PACK == 1 else jnp.concatenate(rows, axis=1)
    whole = scr[...]
    for t in range(NT):
        out_ref[t] = whole


def near(x):
    return pltpu.with_memory_space_constraint(x, pltpu.VMEM)


def copies(pairs):
    return pl.pallas_call(
        copies_kernel,
        out_shape=pltpu.VMEM((NT, 8, 128), jnp.float32),
        scratch_shapes=[pltpu.VMEM((8, 128), jnp.float32)],
        name="copies",
    )(near(pairs))


GROUP = 8
ROWS = 512 // PACK


def total_kernel(where_ref, w_ref, p_ref, out_ref, turned, tot):
    whole = w_ref[...].reshape(ROWS, 128)
    for n in range(ROWS // 128):
        turned[:, 128 * n : 128 * n + 128] = jnp.transpose(whole[128 * n : 128 * n + 128, :])
    digit = lax.broadcasted_iota(jnp.int32, (16, ROWS), 0).astype(jnp.float32)
    row = lax.broadcasted_iota(jnp.int32, (128, 128), 0)
    lane = lanes((128, 128))
    own = (row // 16) == (lane // 16)
    spot = (row % 8) == (lane // 16)
    for k0 in range(0, NB, GROUP):
        acc = jnp.zeros((128, 128), jnp.float32)
        for i in range(PACK):
            parts = ([], [], [])
            right = []
            at = i * 2 * NB + k0
            val = turned[at : at + GROUP, :]
            off = turned[at + NB : at + NB + GROUP, :]
            first = val.astype(jnp.bfloat16).astype(jnp.float32)
            rest = val - first
            second = rest.astype(jnp.bfloat16).astype(jnp.float32)
            third = rest - second
            hi = jnp.floor(off * 0.0625)
            lo = off - 16.0 * hi
            for k in range(GROUP):
                hot = digit == hi[k : k + 1, :]
                for m, part in enumerate((first, second, third)):
                    parts[m].append(jnp.where(hot, part[k : k + 1, :], 0.0).astype(jnp.bfloat16))
                right.append(jnp.where(digit == lo[k : k + 1, :], 1.0, 0.0).astype(jnp.bfloat16))
            right = jnp.concatenate(right, axis=0)
            for m in range(3):
                acc += lax.dot_general(
                    jnp.concatenate(parts[m], axis=0),
                    right,
                    (((1,), (1,)), ((), ())),
                    preferred_element_type=jnp.float32,
                )
        acc = jnp.where(own, acc, 0.0)
        for turn in (64, 32, 16):
            acc = acc + pltpu.roll(acc, turn, 1)
        acc = jnp.where(spot, acc, 0.0)
        tot[2 * k0 : 2 * k0 + 16, :] = jnp.sum(acc.reshape(16, 8, 128), axis=1)
    new = p_ref[...] - STEP * tot[...]
    for s in range(2 * NS):
        out_ref[s] = new


def total(where, pairs, params):
    rows = 2 * NB
    return pl.pallas_call(
        total_kernel,
        grid_spec=pltpu.PrefetchScalarGridSpec(
            num_scalar_prefetch=1,
            grid=(1,),
            in_specs=[
                pl.BlockSpec((NT, 8, 128), lambda i, at: (0, 0, 0)),
                pl.BlockSpec((rows, 128), lambda i, at: (at[0], 0)),
            ],
            out_specs=pl.BlockSpec((2 * NS, rows, 128), lambda i, at: (0, 0, 0)),
            scratch_shapes=[pltpu.VMEM((128, ROWS), jnp.float32), pltpu.VMEM((rows, 128), jnp.float32)],
        ),
        out_shape=pltpu.VMEM((2 * NS, rows, 128), jnp.float32),
        name="total",
    )(where, near(pairs), params)


def shards(gradient, residual, indices, params):
    g = gradient.reshape(1024, 128)
    r = residual.reshape(1024, 128)
    idx = indices.reshape(4, 128)
    where = (lax.axis_index("outer") * NS + lax.axis_index(NEAR)).reshape(1).astype(jnp.int32)
    where, idx = lax.optimization_barrier((where, idx))
    send, res = pick(idx, g, r)
    got = lax.all_to_all(send, NEAR + ("outer",), 0, 0)
    everyone = lax.all_to_all(copies(got), FAR, 0, 0)
    new = total(where, everyone, params.reshape(1024, 128))
    both = lax.all_to_all(new, ("outer",) + NEAR, 0, 0)
    return both.reshape(131072), res.reshape(1, 131072)


def solution(mesh):
    torus = Mesh(mesh.devices.reshape((2,) * 9), AXES)
    placed = (P(AXES, None), P(AXES, None), P(AXES, None), P())
    return jax.shard_map(
        shards, mesh=torus, in_specs=placed, out_specs=(P(), P(AXES, None)), check_vma=False
    )
```

```python
import jax
import jax.numpy as jnp
from jax import lax
from jax.experimental import pallas as pl
from jax.experimental.pallas import tpu as pltpu
from jax.sharding import Mesh
from jax.sharding import PartitionSpec as P

AXES = ("x1", "x0", "y2", "y1", "y0", "z2", "z1", "z0", "outer")
NEAR = ("x1", "x0", "y0")
FAR = tuple(a for a in AXES if a not in NEAR and a != "outer")
NS = 2 ** len(NEAR)
NT = 2 ** len(FAR)
NB = 256 // NS
PACK = 64 // NB
STEP = 0.5


def lanes(shape):
    return lax.broadcasted_iota(jnp.int32, shape, 1)


def pick_kernel(idx_ref, g_hbm, r_hbm, send_ref, res_hbm, g_ref, r_ref, res_ref, v_scr, o_scr, col_scr, g_sem, r_sem, res_sem):
    def span(n):
        return pl.ds(256 * n, 256)

    loads = []
    for n in range(4):
        one = pltpu.make_async_copy(g_hbm.at[span(n)], g_ref.at[span(n)], g_sem.at[n])
        two = pltpu.make_async_copy(r_hbm.at[span(n)], r_ref.at[span(n)], r_sem.at[n])
        one.start()
        two.start()
        loads.append((one, two))
    for n in range(4):
        off = (idx_ref[n : n + 1, :] & 255).astype(jnp.float32)
        o_scr[n : n + 1, :] = off
        col_scr[n] = jnp.transpose(jnp.broadcast_to(off, (128, 128)))
    lane = lanes((128, 128)).astype(jnp.float32)
    stores = []
    for n in range(4):
        for load in loads[n]:
            load.wait()
        col = col_scr[n]
        low = col == lane
        high = col == lane + 128.0
        even = pl.ds(256 * n, 128, stride=2)
        odd = pl.ds(256 * n + 1, 128, stride=2)
        a0 = g_ref[even, :] + r_ref[even, :]
        a1 = g_ref[odd, :] + r_ref[odd, :]
        res_ref[even, :] = jnp.where(low, 0.0, a0)
        res_ref[odd, :] = jnp.where(high, 0.0, a1)
        store = pltpu.make_async_copy(res_ref.at[span(n)], res_hbm.at[span(n)], res_sem.at[n])
        store.start()
        stores.append(store)
        hit = jnp.where(low, a0, jnp.where(high, a1, 0.0))
        v_scr[n : n + 1, :] = jnp.sum(jnp.transpose(hit), axis=0, keepdims=True)
    lane1 = lanes((1, 128))
    for s in range(NS):
        for c in range(2):
            block = c * 256 + s * NB
            row, at = block // 128, block % 128
            val = v_scr[row : row + 1, :]
            offs = o_scr[row : row + 1, :]
            left = pltpu.roll(val, (128 - at) % 128, 1) if at else val
            move = (NB - at) % 128
            right = pltpu.roll(offs, move, 1) if move else offs
            send_ref[c * NS + s] = jnp.where(lane1 < NB, left, right)[:, : 2 * NB]
    for store in stores:
        store.wait()


def pick(idx, g, r):
    in_hbm = pl.BlockSpec(memory_space=pltpu.HBM)
    in_vmem = pl.BlockSpec(memory_space=pltpu.VMEM)
    return pl.pallas_call(
        pick_kernel,
        in_specs=[in_vmem, in_hbm, in_hbm],
        out_specs=[in_vmem, in_hbm],
        out_shape=[
            pltpu.VMEM((2 * NS, 1, 2 * NB), jnp.float32),
            jax.ShapeDtypeStruct((1024, 128), jnp.float32),
        ],
        scratch_shapes=[
            pltpu.VMEM((1024, 128), jnp.float32),
            pltpu.VMEM((1024, 128), jnp.float32),
            pltpu.VMEM((1024, 128), jnp.float32),
            pltpu.VMEM((4, 128), jnp.float32),
            pltpu.VMEM((4, 128), jnp.float32),
            pltpu.VMEM((4, 128, 128), jnp.float32),
            pltpu.SemaphoreType.DMA((4,)),
            pltpu.SemaphoreType.DMA((4,)),
            pltpu.SemaphoreType.DMA((4,)),
        ],
        name="pick",
    )(idx, g, r)


def copies_kernel(in_ref, out_ref, scr):
    for p in range(8):
        rows = [in_ref[p + 8 * i] for i in range(PACK)]
        scr[p : p + 1, :] = rows[0] if PACK == 1 else jnp.concatenate(rows, axis=1)
    whole = scr[...]
    for t in range(NT):
        out_ref[t] = whole


def near(x):
    return pltpu.with_memory_space_constraint(x, pltpu.VMEM)


def copies(pairs):
    return pl.pallas_call(
        copies_kernel,
        out_shape=pltpu.VMEM((NT, 8, 128), jnp.float32),
        scratch_shapes=[pltpu.VMEM((8, 128), jnp.float32)],
        name="copies",
    )(near(pairs))


GROUP = 8
ROWS = 512 // PACK


def total_kernel(where_ref, w_ref, p_ref, out_ref, turned, tot):
    whole = w_ref[...].reshape(ROWS, 128)
    for n in range(ROWS // 128):
        turned[:, 128 * n : 128 * n + 128] = jnp.transpose(whole[128 * n : 128 * n + 128, :])
    digit = lax.broadcasted_iota(jnp.int32, (16, ROWS), 0).astype(jnp.float32)
    row = lax.broadcasted_iota(jnp.int32, (128, 128), 0)
    lane = lanes((128, 128))
    own = (row // 16) == (lane // 16)
    spot = (row % 8) == (lane // 16)
    for k0 in range(0, NB, GROUP):
        acc = jnp.zeros((128, 128), jnp.float32)
        for i in range(PACK):
            parts = ([], [], [])
            right = []
            at = i * 2 * NB + k0
            val = turned[at : at + GROUP, :]
            off = turned[at + NB : at + NB + GROUP, :]
            first = val.astype(jnp.bfloat16).astype(jnp.float32)
            rest = val - first
            second = rest.astype(jnp.bfloat16).astype(jnp.float32)
            third = rest - second
            hi = jnp.floor(off * 0.0625)
            lo = off - 16.0 * hi
            for k in range(GROUP):
                hot = digit == hi[k : k + 1, :]
                for m, part in enumerate((first, second, third)):
                    parts[m].append(jnp.where(hot, part[k : k + 1, :], 0.0).astype(jnp.bfloat16))
                right.append(jnp.where(digit == lo[k : k + 1, :], 1.0, 0.0).astype(jnp.bfloat16))
            right = jnp.concatenate(right, axis=0)
            for m in range(3):
                acc += lax.dot_general(
                    jnp.concatenate(parts[m], axis=0),
                    right,
                    (((1,), (1,)), ((), ())),
                    preferred_element_type=jnp.float32,
                )
        acc = jnp.where(own, acc, 0.0)
        for turn in (64, 32, 16):
            acc = acc + pltpu.roll(acc, turn, 1)
        acc = jnp.where(spot, acc, 0.0)
        tot[2 * k0 : 2 * k0 + 16, :] = jnp.sum(acc.reshape(16, 8, 128), axis=1)
    new = p_ref[...] - STEP * tot[...]
    for s in range(2 * NS):
        out_ref[s] = new


def total(where, pairs, params):
    rows = 2 * NB
    return pl.pallas_call(
        total_kernel,
        grid_spec=pltpu.PrefetchScalarGridSpec(
            num_scalar_prefetch=1,
            grid=(1,),
            in_specs=[
                pl.BlockSpec((NT, 8, 128), lambda i, at: (0, 0, 0)),
                pl.BlockSpec((rows, 128), lambda i, at: (at[0], 0)),
            ],
            out_specs=pl.BlockSpec((2 * NS, rows, 128), lambda i, at: (0, 0, 0)),
            scratch_shapes=[pltpu.VMEM((128, ROWS), jnp.float32), pltpu.VMEM((rows, 128), jnp.float32)],
        ),
        out_shape=pltpu.VMEM((2 * NS, rows, 128), jnp.float32),
        name="total",
    )(where, near(pairs), params)


def shards(gradient, residual, indices, params):
    g = gradient.reshape(1024, 128)
    r = residual.reshape(1024, 128)
    idx = indices.reshape(4, 128)
    where = (lax.axis_index("outer") * NS + lax.axis_index(NEAR)).reshape(1).astype(jnp.int32)
    where, idx = lax.optimization_barrier((where, idx))
    send, res = pick(idx, g, r)
    got = lax.all_to_all(send, ("outer",) + NEAR, 0, 0)
    everyone = lax.all_to_all(copies(got), FAR, 0, 0)
    new = total(where, everyone, params.reshape(1024, 128))
    both = lax.all_to_all(new, ("outer",) + NEAR, 0, 0)
    return both.reshape(131072), res.reshape(1, 131072)


def solution(mesh):
    torus = Mesh(mesh.devices.reshape((2,) * 9), AXES)
    placed = (P(AXES, None), P(AXES, None), P(AXES, None), P())
    return jax.shard_map(
        shards, mesh=torus, in_specs=placed, out_specs=(P(), P(AXES, None)), check_vma=False
    )
```
